512 devices in a mesh: seq: 128 (over y, z_lo, x), tp: 4 (over z_hi, core).
Axes of the slice: x: 4, y: 4, z: 16 (z_hi: 2, z_lo: 8; z = z_hi * 8 + z_lo), core: 2. Of those that a mesh axis runs over, the one named last changes fastest.
Arguments:
- queries: bfloat16 [6144, 2048], P('seq', 'tp'), may hold values from -16 to 16
- keys: bfloat16 [6144, 2048], P('seq', 'tp'), may hold values from -16 to 16
- values: bfloat16 [6144, 2048], P('seq', 'tp'), may hold values from -6 to 6
- patch_stream: bfloat16 [6144, 4096], P('seq', 'tp'), may hold values from -6 to 6
- out_weight: bfloat16 [2048, 4096], P('tp', 'seq'), may hold values from -1 to 1
- down_weight: bfloat16 [4096, 1280], P('tp'), may hold values from -0.09375 to 0.09375
- byte_states: bfloat16 [24576, 1280], P('seq', 'tp'), may hold values from -6 to 6
- patch_starts: int32 [128, 48], P('seq'), may hold values from 0 to 192, as said below
Outputs:
- new_patches: bfloat16 [6144, 4096], P('seq', 'tp')
- new_bytes: bfloat16 [24576, 1280], P('seq', 'tp')
The draws below stay inside these ranges and needn't reach their ends.
Inputs may be any that keep to these rules, and one draw needn't show every extreme that they name: `patch_starts`: each row d lists rising offsets within device d's 192 bytes at which patches start: the first is 0 in row 0 and from 4 to 7 in the other rows, the others are 8 or more; at least 24 entries of a row are offsets, some row has all 48, and the remaining entries at the end of a row equal 192.
All inputs are finite; a program needn't handle non-finite values.
Results may differ from the reference program's by a relative error of at most 0.015.
Values may be sent and summed in bfloat16 or wider, within the bound.
No kernel may reach another device: no remote copies, remote signals or barrier semaphores. Data moves between devices by JAX's collectives and lax.ppermute only.
A program may use at most 128 MiB of HBM per device.

```python
import jax
import jax.numpy as jnp
from jax import lax

D = 4096
DL = 1280
HEADS = 16
DH = 128
B_DEV = 192
EDGE = 8
P_CAP = 48
HW = 2048
PATCHES = 6144
BYTES = 24576
N_SEQ = 128


def drawn_rows(key, salt):
    return jnp.clip(jax.random.normal(jax.random.fold_in(key, salt), (PATCHES, HW), jnp.float32), -6.0, 6.0)


def draw_queries(key, part):
    rows = drawn_rows(key, 1)
    return rows.astype(jnp.bfloat16)


def draw_keys(key, part):
    rows = drawn_rows(key, 2)
    return rows.astype(jnp.bfloat16)


def draw_patch_starts(key, part):
    inner = jax.random.fold_in(key, 11)
    count_key, first_key, pick_key, full_key, edge_key = jax.random.split(inner, 5)
    device = jnp.arange(N_SEQ, dtype=jnp.int32)
    counts = jax.random.randint(count_key, (N_SEQ,), P_CAP // 2, P_CAP + 1)
    full_device = jax.random.randint(full_key, (), 0, N_SEQ)
    counts = jnp.where(device == full_device, P_CAP, counts)
    firsts = jax.random.randint(first_key, (N_SEQ,), EDGE // 2, EDGE)
    edge_device = jax.random.randint(edge_key, (), 1, N_SEQ)
    firsts = jnp.where(device == edge_device, EDGE - 1, firsts)
    firsts = jnp.where(device == 0, 0, firsts)

    def one_row(row_key, count, first):
        order = jax.random.permutation(row_key, B_DEV - EDGE)[:P_CAP - 1] + EDGE
        place = jnp.arange(P_CAP - 1, dtype=jnp.int32)
        rest = jnp.where(place < count - 1, order, B_DEV)
        rest = jnp.sort(rest)
        return jnp.concatenate([first[None], rest]).astype(jnp.int32)
    row_keys = jax.random.split(pick_key, N_SEQ)
    return jax.vmap(one_row)(row_keys, counts, firsts)


def levels(rng, dims, cuts, least, largest):
    factor_of = 1.0
    for dim, parts in cuts:
        draws = jax.random.uniform(jax.random.fold_in(jax.random.fold_in(rng, 6), dim), (parts,), jnp.float32, least / len(cuts), largest / len(cuts))
        factor_of = factor_of * jnp.repeat(jnp.exp(draws), dims[dim] // parts).reshape((-1,) + (1,) * (len(dims) - 1 - dim))
    return factor_of


def gaussian(rng, shape, width, bound, cuts=(), kind=jnp.bfloat16):
    level = levels(rng, shape, cuts, -0.22, 0.18) if cuts else 1.0
    array = jax.random.normal(rng, shape, jnp.float32) * width * level
    return jnp.minimum(jnp.maximum(array, -bound), bound).astype(kind)


def setup_inputs(seed: int = 0) -> dict:
    streams_of = jax.random.split(jax.random.key(seed), 9)
    queries = draw_queries(jax.random.fold_in(streams_of[8], 71), 0)
    keys = draw_keys(jax.random.fold_in(streams_of[8], 71), 0)
    values = gaussian(streams_of[2], (PATCHES, HW), 1.0, 6.0, ((0, 128), (1, 4)))
    patch_stream = gaussian(streams_of[3], (PATCHES, D), 1.0, 6.0, ((0, 128), (1, 4)))
    out_weight = gaussian(streams_of[4], (HW, D), (HW // 64) ** -0.5, 1.0, ((0, 4), (1, 128)))
    down_weight = gaussian(streams_of[5], (D, DL), D ** -0.5, 0.09375, ((0, 4),))
    byte_states = gaussian(streams_of[6], (BYTES, DL), 1.0, 6.0, ((0, 128), (1, 4)))
    patch_starts = draw_patch_starts(jax.random.fold_in(streams_of[8], 71), 0)
    return dict(queries=queries, keys=keys, values=values, patch_stream=patch_stream, out_weight=out_weight, down_weight=down_weight, byte_states=byte_states, patch_starts=patch_starts)


NEG = -1.0e30


def reference(queries, keys, values, patch_stream, out_weight, down_weight, byte_states, patch_starts):
    total_slots = queries.shape[0]
    valid = (patch_starts.reshape(-1) < B_DEV)
    slot_ids = jnp.arange(total_slots, dtype=jnp.int32)
    key_heads = keys.reshape(total_slots, HEADS, DH).astype(jnp.float32)
    value_heads = values.reshape(total_slots, HEADS, DH).astype(jnp.float32)
    block_rows = 256 if total_slots % 256 == 0 else P_CAP
    scale = DH ** -0.5

    def one_block(index):
        begin = (index * block_rows).astype(jnp.int32)
        query_block = lax.dynamic_slice_in_dim(queries, begin, block_rows, 0)
        query_heads = query_block.reshape(block_rows, HEADS, DH).astype(jnp.float32)
        scores = jnp.einsum("qhd,khd->hqk", query_heads, key_heads) * scale
        query_ids = begin + jnp.arange(block_rows, dtype=jnp.int32)
        allowed = valid[None, :] & (slot_ids[None, :] <= query_ids[:, None])
        scores = jnp.where(allowed[None], scores, NEG)
        peak = jnp.max(scores, axis=-1, keepdims=True)
        expo = jnp.where(allowed[None], jnp.exp(scores - peak), 0.0)
        total = jnp.sum(expo, axis=-1)
        weights = expo.astype(jnp.bfloat16).astype(jnp.float32)
        summed = jnp.einsum("hqk,khd->qhd", weights, value_heads)
        result = summed / jnp.transpose(total)[:, :, None]
        return result.reshape(block_rows, HEADS * DH).astype(jnp.bfloat16)

    attn = lax.map(one_block, jnp.arange(total_slots // block_rows, dtype=jnp.int32))
    attn = attn.reshape(total_slots, HEADS * DH)
    mixed = jnp.dot(attn, out_weight, preferred_element_type=jnp.float32)
    new_patches = (patch_stream.astype(jnp.float32) + mixed).astype(jnp.bfloat16)
    patch_down = jnp.dot(new_patches, down_weight, preferred_element_type=jnp.float32).astype(jnp.bfloat16)

    valid_rows = patch_starts < B_DEV
    counts = jnp.sum(valid_rows.astype(jnp.int32), axis=1)
    position = jnp.arange(B_DEV, dtype=jnp.int32)
    below = jnp.sum((patch_starts[:, None, :] <= position[None, :, None]).astype(jnp.int32), axis=2)
    device = jnp.arange(patch_starts.shape[0], dtype=jnp.int32)[:, None]
    prev_slot = (device - 1) * P_CAP + jnp.roll(counts, 1)[:, None] - 1
    owner = jnp.where(below > 0, device * P_CAP + below - 1, prev_slot)
    owner = jnp.maximum(owner, 0).astype(jnp.int32)
    gathered = jnp.take(patch_down, owner.reshape(-1), axis=0)
    new_bytes = (byte_states.astype(jnp.float32) + gathered.astype(jnp.float32)).astype(jnp.bfloat16)
    return new_patches, new_bytes
```

```python
import jax
import jax.numpy as jnp
from jax import lax
from jax.experimental import pallas as pl
from jax.experimental.pallas import tpu as pltpu
from jax.sharding import Mesh
from jax.sharding import PartitionSpec as P

DH = 128
B_DEV = 192
SEQ = ("y", "z", "x")
TP = ("h", "c")
PLANE = ("y", "x")
ROWS = 48
PAD = 56
NEG = -1e30
FLOOR = -1e29
MARK = 64.0
LIMIT = 4096.0
FAR = 1 << 30


def pieces(value):
    first = value.astype(jnp.bfloat16)
    rest = value - first.astype(jnp.float32)
    second = rest.astype(jnp.bfloat16)
    third = (rest - second.astype(jnp.float32)).astype(jnp.bfloat16)
    return [first, second, third]


def attend_kernel(place_ref, key_ids_ref, q_ref, near_ref, far_ref, out_ref):
    blocks, rows, width = q_ref.shape
    heads = width // DH
    kv = jnp.concatenate([near_ref[...].reshape(-1, 2 * width), far_ref[...].reshape(-1, 2 * width)], axis=0)
    ones = jnp.ones((8, DH), jnp.bfloat16)
    nt = (((1,), (1,)), ((), ()))
    marks = lax.dot_general(ones, kv[:, :DH], nt, preferred_element_type=jnp.float32)[:1]
    key_ids = jnp.where(marks > LIMIT, FAR, key_ids_ref[...] + place_ref[0])
    group = 4
    row = lax.rem(lax.broadcasted_iota(jnp.int32, (group * rows, 1), 0), rows)
    step = lax.div(lax.broadcasted_iota(jnp.int32, (group * rows, 1), 0), rows)
    row = jnp.where(row < ROWS, row, -1) + step * ROWS
    lane = lax.broadcasted_iota(jnp.int32, (group * rows, DH), 1)

    def one_group(index, _):
        device = index * 32 + place_ref[1]
        allowed = key_ids <= row + device * ROWS
        stats = jnp.zeros((group * rows, DH), jnp.float32)
        at_blocks = pl.ds(index * group, group)
        for h in range(heads):
            q = q_ref[at_blocks, :, h * DH : (h + 1) * DH].reshape(group * rows, DH)
            k = kv[:, h * DH : (h + 1) * DH]
            v = kv[:, width + h * DH : width + (h + 1) * DH]
            s = lax.dot_general(q, k, nt, preferred_element_type=jnp.float32) * (DH**-0.5)
            s = jnp.where(allowed, s, NEG)
            peak = jnp.maximum(jnp.max(s, axis=1, keepdims=True), FLOOR)
            e = jnp.exp(s - peak)
            total = jnp.sum(e, axis=1, keepdims=True)
            o = jnp.dot(e.astype(jnp.bfloat16), v, preferred_element_type=jnp.float32)
            out_ref[at_blocks, :, h * DH : (h + 1) * DH] = o.astype(jnp.bfloat16).reshape(group, rows, DH)
            for at, part in enumerate(pieces(peak) + pieces(total)):
                stats = jnp.where(lane == h * 6 + at, part.astype(jnp.float32), stats)
        out_ref[at_blocks, :, width:] = stats.astype(jnp.bfloat16).reshape(group, rows, DH)
        return 0

    lax.fori_loop(0, blocks // group, one_group, 0)


def combine_kernel(in_ref, out_ref):
    blocks, rows, width = in_ref.shape
    heads = (width - DH) // DH
    for h in range(heads):
        peaks, totals = [], []
        for b in range(blocks):
            stat = in_ref[b, :, heads * DH :].astype(jnp.float32)
            at = h * 6
            peaks.append(stat[:, at : at + 1] + stat[:, at + 1 : at + 2] + stat[:, at + 2 : at + 3])
            totals.append(stat[:, at + 3 : at + 4] + stat[:, at + 4 : at + 5] + stat[:, at + 5 : at + 6])
        top = peaks[0]
        for b in range(1, blocks):
            top = jnp.maximum(top, peaks[b])
        total = jnp.zeros_like(top)
        summed = jnp.zeros((rows, DH), jnp.float32)
        for b in range(blocks):
            share = jnp.exp(peaks[b] - top)
            total = total + share * totals[b]
            summed = summed + share * in_ref[b, :, h * DH : (h + 1) * DH].astype(jnp.float32)
        total = jnp.where(total > 0, total, 1.0)
        out_ref[:, h * DH : (h + 1) * DH] = (summed / total).astype(jnp.bfloat16)


VM = pl.BlockSpec(memory_space=pltpu.VMEM)
SM = pl.BlockSpec(memory_space=pltpu.SMEM)


def attend(place, key_ids, q, near, far):
    blocks, rows, width = q.shape
    return pl.pallas_call(
        attend_kernel,
        out_shape=jax.ShapeDtypeStruct((blocks, rows, width + DH), jnp.bfloat16),
        in_specs=[SM, VM, VM, VM, VM],
        out_specs=VM,
        cost_estimate=pl.CostEstimate(flops=4_000_000_000, bytes_accessed=3_000_000, transcendentals=1_400_000),
    )(place, key_ids, q, near, far)


def combine(parts):
    _, rows, width = parts.shape
    return pl.pallas_call(
        combine_kernel,
        out_shape=jax.ShapeDtypeStruct((rows, width - DH), jnp.bfloat16),
        in_specs=[VM],
        out_specs=VM,
        cost_estimate=pl.CostEstimate(flops=2_000_000_000, bytes_accessed=1_200_000, transcendentals=4_000),
    )(parts)


def exchange(value, axes):
    return lax.all_to_all(value, axes, split_axis=0, concat_axis=0, tiled=True)


def held_at(distance):
    return (distance & 1) * 4 + (distance & 2) + lax.div(distance, 4)


def project_kernel(place_ref, attn_ref, own_ref, less_ref, more_ref, low_ref, high_ref, stream_ref, down_ref, new_ref, keep_ref, send_ref):
    y, x, c, z = place_ref[0], place_ref[1], place_ref[2], place_ref[3]
    nt = (((1,), (1,)), ((), ()))
    span = 256
    heads = [attn_ref[lax.rem(y + step, 4)] for step in range(4)]
    turns = [lax.rem(x + 4 - source, 4) for source in range(4)]
    for at in range(stream_ref.shape[1] // span):
        total = stream_ref[:, at * span : (at + 1) * span].astype(jnp.float32)
        spots = [(turn, held_at((at * 2 + i) ^ z)) for i in range(2) for turn in turns]
        mixed = jnp.zeros_like(total)
        for attn, refs in zip(heads, ((own_ref,), (more_ref,), (low_ref, high_ref), (less_ref,))):
            weight = jnp.concatenate([ref[turn, spot] for turn, spot in spots for ref in refs], axis=0)
            mixed = mixed + lax.dot_general(attn, weight, nt, preferred_element_type=jnp.float32)
        new_ref[:, at * span : (at + 1) * span] = (total + mixed).astype(jnp.bfloat16)
    down = jnp.dot(new_ref[...], down_ref[...], preferred_element_type=jnp.float32)
    for half in range(2):
        at = half * 640
        first, second = down[:, at : at + 320], down[:, at + 320 : at + 640]
        keep_ref[half] = jnp.where(c == 0, first, second)
        send_ref[half] = jnp.where(c == 0, second, first).astype(jnp.bfloat16)


def project(place, attn, weights, stream, down_weight):
    rows, width = stream.shape
    return pl.pallas_call(
        project_kernel,
        out_shape=(
            jax.ShapeDtypeStruct((rows, width), jnp.bfloat16),
            jax.ShapeDtypeStruct((2, rows, 320), jnp.float32),
            jax.ShapeDtypeStruct((2, rows, 320), jnp.bfloat16),
        ),
        in_specs=[SM] + [VM] * 8,
        out_specs=(VM, VM, VM),
        cost_estimate=pl.CostEstimate(flops=4_000_000_000, bytes_accessed=7_000_000, transcendentals=0),
    )(place, attn, *weights, stream, down_weight)


def turned(value, axis, by):
    return lax.ppermute(value, axis, [(i, (i + by) % 4) for i in range(4)])


def line_halves(block):
    held = block[None]
    for bit in (4, 2, 1):
        other = lax.ppermute(held, "z", [(i, i ^ bit) for i in range(8)])
        if bit == 1:
            return held, other
        held = jnp.concatenate([held, other], axis=0)


def plane_gathered(blocks):
    own = jnp.stack([blocks] + [turned(blocks, "x", k) for k in (1, 2, 3)])
    less, more = turned(own, "y", 1), turned(own, "y", -1)
    return own, less, more, turned(less[:, :, :16], "y", 1), turned(more[:, :, 16:], "y", -1)


def across(value, axis):
    return lax.ppermute(value, axis, [(0, 1), (1, 0)])


def on_device(queries, keys, values, patch_stream, out_weight, down_weight, byte_states, patch_starts):
    y, z, x, h, c = (lax.axis_index(a) for a in (*SEQ, *TP))
    starts = patch_starts.reshape(-1)
    valid = starts < B_DEV
    count = jnp.sum(valid.astype(jnp.int32))
    pairs = [(a * 4 + t, t * 4 + a) for a in range(4) for t in range(4)]
    block = lax.ppermute(out_weight.T, ("y", "h", "c"), pairs)
    marked = jnp.where(valid[:, None], keys, jnp.bfloat16(MARK))
    kv = jnp.concatenate([marked, values], axis=1)
    blocks = jnp.concatenate(line_halves(block), axis=0)

    last = lax.dynamic_slice(jnp.concatenate([queries, patch_stream], axis=1), (count - 1, 0), (1, 1536))
    pairs = [(i, i + 1) for i in range(127)]
    earlier = lax.ppermute(last, SEQ, pairs)
    weights = plane_gathered(blocks)
    near, far = line_halves(kv)
    q = jnp.concatenate([queries, earlier[:, :512], jnp.zeros((PAD - ROWS - 1, 512), jnp.bfloat16)], axis=0)
    stream = jnp.concatenate([patch_stream, earlier[:, 512:], jnp.zeros((PAD - ROWS - 1, 1024), jnp.bfloat16)], axis=0)
    q = exchange(jnp.broadcast_to(q[None], (16, *q.shape)), PLANE)

    place = jnp.stack([(y * 32 + x) * ROWS, z * 4]).astype(jnp.int32)
    slot = jnp.arange(8 * ROWS, dtype=jnp.int32)
    away = slot // ROWS
    away = (away & 1) * 4 + (away & 2) + (away >> 2)
    key_ids = ((away ^ z) * (4 * ROWS) + slot % ROWS)[None]
    attn = combine(exchange(attend(place, key_ids, q, near, far), PLANE))

    attn = lax.all_gather(attn, TP, axis=0)
    new_rows, keep, send = project(jnp.stack([y, x, c, z]), attn, weights, stream, down_weight)
    both = keep + across(send, "c").astype(jnp.float32)
    here = jnp.where(h == 0, both[0], both[1])
    there = jnp.where(h == 0, both[1], both[0]).astype(jnp.bfloat16)
    patch_down = (here + across(there, "h").astype(jnp.float32)).astype(jnp.bfloat16)

    position = jnp.arange(B_DEV, dtype=jnp.int32)[:, None]
    begins = jnp.concatenate([starts, jnp.zeros((1,), jnp.int32), jnp.full((PAD - ROWS - 1,), B_DEV, jnp.int32)])
    ends = jnp.concatenate([starts[1:], jnp.full((1,), B_DEV, jnp.int32), starts[:1], jnp.full((PAD - ROWS - 1,), B_DEV, jnp.int32)])
    member = ((begins[None, :] <= position) & (position < ends[None, :])).astype(jnp.bfloat16)
    added = jnp.dot(member, patch_down, preferred_element_type=jnp.float32)
    new_bytes = (byte_states.astype(jnp.float32) + added).astype(jnp.bfloat16)
    return (new_rows[:ROWS], new_bytes)


def solution(mesh):
    split = Mesh(mesh.devices.reshape(4, 8, 4, 2, 2), ("y", "z", "x", "h", "c"))
    return jax.shard_map(
        on_device,
        mesh=split,
        in_specs=(
            P(SEQ, TP),
            P(SEQ, TP),
            P(SEQ, TP),
            P(SEQ, TP),
            P(TP, SEQ),
            P(TP, None),
            P(SEQ, TP),
            P(SEQ, None),
        ),
        out_specs=(P(SEQ, TP), P(SEQ, TP)),
        check_vma=False,
    )
```

```python
import jax
import jax.numpy as jnp
from jax import lax
from jax.experimental import pallas as pl
from jax.experimental.pallas import tpu as pltpu
from jax.sharding import Mesh
from jax.sharding import PartitionSpec as P


DH = 128
B_DEV = 192
SEQ = ("y", "z", "x")
TP = ("h", "c")
PLANE = ("y", "x")
ROWS = 48
PAD = 56
NEG = -1e30
FLOOR = -1e29
MARK = 64.0
LIMIT = 4096.0
FAR = 1 << 30


def prepare_kernel(starts_ref, keys_ref, values_ref, queries_ref, stream_ref, kv_ref, last_ref):
    rows = keys_ref.shape[0]
    valid = (starts_ref[...] < B_DEV).astype(jnp.float32)
    count = jnp.sum(valid, axis=1, keepdims=True)
    row = lax.broadcasted_iota(jnp.int32, (rows, rows), 0)
    lane = lax.broadcasted_iota(jnp.int32, (rows, rows), 1)
    held = jnp.sum(jnp.where(row == lane, valid, 0.0), axis=1, keepdims=True)
    width = keys_ref.shape[1]
    kv_ref[0, :, :width] = jnp.where(held > 0, keys_ref[...], jnp.full_like(keys_ref, MARK))
    kv_ref[0, :, width:] = values_ref[...]
    lane = lax.broadcasted_iota(jnp.int32, (1, rows), 1).astype(jnp.float32)
    pick = (lane == count - 1).astype(jnp.bfloat16)
    last_ref[:, :width] = jnp.dot(pick, queries_ref[...], preferred_element_type=jnp.float32).astype(jnp.bfloat16)
    last_ref[:, width:] = jnp.dot(pick, stream_ref[...], preferred_element_type=jnp.float32).astype(jnp.bfloat16)


def attend_kernel(place_ref, key_ids_ref, q_ref, near_ref, far_ref, out_ref):
    blocks, rows, width = q_ref.shape
    heads = width // DH
    kv = jnp.concatenate([near_ref[...].reshape(-1, 2 * width), far_ref[...].reshape(-1, 2 * width)], axis=0)
    ones = jnp.ones((8, DH), jnp.bfloat16)
    nt = (((1,), (1,)), ((), ()))
    marks = lax.dot_general(ones, kv[:, :DH], nt, preferred_element_type=jnp.float32)[:1]
    key_ids = jnp.where(marks > LIMIT, FAR, key_ids_ref[...] + place_ref[0])
    group = 4
    row = lax.rem(lax.broadcasted_iota(jnp.int32, (group * rows, 1), 0), rows)
    step = lax.div(lax.broadcasted_iota(jnp.int32, (group * rows, 1), 0), rows)
    row = jnp.where(row < ROWS, row, -1) + step * ROWS
    lane = lax.broadcasted_iota(jnp.int32, (group * rows, DH), 1)

    def one_group(index, _):
        device = index * 32 + place_ref[1]
        allowed = key_ids <= row + device * ROWS
        stats = jnp.zeros((group * rows, DH), jnp.float32)
        at_blocks = pl.ds(index * group, group)
        for h in range(heads):
            q = q_ref[at_blocks, :, h * DH : (h + 1) * DH].reshape(group * rows, DH)
            k = kv[:, h * DH : (h + 1) * DH]
            v = kv[:, width + h * DH : width + (h + 1) * DH]
            s = lax.dot_general(q, k, nt, preferred_element_type=jnp.float32) * (DH**-0.5)
            s = jnp.where(allowed, s, NEG)
            peak = jnp.maximum(jnp.max(s, axis=1, keepdims=True), FLOOR).astype(jnp.bfloat16).astype(jnp.float32)
            e = jnp.exp(s - peak)
            total = jnp.sum(e, axis=1, keepdims=True)
            o = jnp.dot(e.astype(jnp.bfloat16), v, preferred_element_type=jnp.float32)
            out_ref[at_blocks, :, h * DH : (h + 1) * DH] = o.astype(jnp.bfloat16).reshape(group, rows, DH)
            coarse = total.astype(jnp.bfloat16).astype(jnp.float32)
            for at, part in enumerate((peak, coarse, total - coarse)):
                stats = jnp.where(lane == h * 3 + at, part, stats)
        out_ref[at_blocks, :, width:] = stats.astype(jnp.bfloat16).reshape(group, rows, DH)
        return 0

    lax.fori_loop(0, blocks // group, one_group, 0)


def combine_kernel(in_ref, out_ref):
    blocks, rows, width = in_ref.shape
    heads = (width - DH) // DH
    stats = [in_ref[b, :, heads * DH :].astype(jnp.float32) for b in range(blocks)]
    top = stats[0]
    for b in range(1, blocks):
        top = jnp.maximum(top, stats[b])
    shares = [jnp.exp(jnp.minimum(stat - top, 0.0)) for stat in stats]
    total = jnp.zeros_like(top)
    for share, stat in zip(shares, stats):
        total = total + share * (pltpu.roll(stat, DH - 1, 1) + pltpu.roll(stat, DH - 2, 1))
    scale = 1.0 / jnp.where(total > 0, total, 1.0)
    for h in range(heads):
        at = slice(h * DH, (h + 1) * DH)
        summed = jnp.zeros((rows, DH), jnp.float32)
        for b in range(blocks):
            summed = summed + shares[b][:, h * 3 : h * 3 + 1] * in_ref[b, :, at].astype(jnp.float32)
        out_ref[:, at] = (summed * scale[:, h * 3 : h * 3 + 1]).astype(jnp.bfloat16)


VM = pl.BlockSpec(memory_space=pltpu.VMEM)
SM = pl.BlockSpec(memory_space=pltpu.SMEM)


def prepare(starts, keys, values, queries, stream):
    rows, width = keys.shape
    return pl.pallas_call(
        prepare_kernel,
        out_shape=(
            jax.ShapeDtypeStruct((1, rows, 2 * width), jnp.bfloat16),
            jax.ShapeDtypeStruct((1, width + stream.shape[1]), jnp.bfloat16),
        ),
        in_specs=[VM] * 5,
        out_specs=(VM, VM),
        cost_estimate=pl.CostEstimate(flops=1_000_000, bytes_accessed=400_000, transcendentals=0),
    )(starts, keys, values, queries, stream)


def attend(place, key_ids, q, near, far):
    blocks, rows, width = q.shape
    return pl.pallas_call(
        attend_kernel,
        out_shape=jax.ShapeDtypeStruct((blocks, rows, width + DH), jnp.bfloat16),
        in_specs=[SM, VM, VM, VM, VM],
        out_specs=VM,
        cost_estimate=pl.CostEstimate(flops=4_000_000_000, bytes_accessed=3_000_000, transcendentals=1_400_000),
    )(place, key_ids, q, near, far)


def combine(parts):
    _, rows, width = parts.shape
    return pl.pallas_call(
        combine_kernel,
        out_shape=jax.ShapeDtypeStruct((rows, width - DH), jnp.bfloat16),
        in_specs=[VM],
        out_specs=VM,
        cost_estimate=pl.CostEstimate(flops=2_000_000_000, bytes_accessed=1_200_000, transcendentals=4_000),
    )(parts)


def exchange(value, axes):
    return lax.all_to_all(value, axes, split_axis=0, concat_axis=0, tiled=True)


def held_at(distance):
    return (distance & 1) * 4 + (distance & 2) + lax.div(distance, 4)


def project_kernel(place_ref, attn_ref, own_ref, less_ref, more_ref, low_ref, high_ref, stream_ref, down_ref, out_ref, keep_ref, send_ref, new_ref):
    y, x, c, z = place_ref[0], place_ref[1], place_ref[2], place_ref[3]
    nt = (((1,), (1,)), ((), ()))
    span = 256
    heads = [attn_ref[lax.rem(y + step, 4)] for step in range(4)]
    turns = [lax.rem(x + 4 - source, 4) for source in range(4)]
    for at in range(stream_ref.shape[1] // span):
        total = stream_ref[:, at * span : (at + 1) * span].astype(jnp.float32)
        spots = [(turn, held_at((at * 2 + i) ^ z)) for i in range(2) for turn in turns]
        mixed = jnp.zeros_like(total)
        for attn, refs in zip(heads, ((own_ref,), (more_ref,), (low_ref, high_ref), (less_ref,))):
            weight = jnp.concatenate([ref[turn, spot] for turn, spot in spots for ref in refs], axis=0)
            mixed = mixed + lax.dot_general(attn, weight, nt, preferred_element_type=jnp.float32)
        new_ref[:, at * span : (at + 1) * span] = (total + mixed).astype(jnp.bfloat16)
    out_ref[...] = new_ref[:ROWS]
    down = jnp.dot(new_ref[...], down_ref[...], preferred_element_type=jnp.float32)
    for half in range(2):
        at = half * 640
        first, second = down[:, at : at + 320], down[:, at + 320 : at + 640]
        keep_ref[half] = jnp.where(c == 0, first, second)
        send_ref[half] = jnp.where(c == 0, second, first).astype(jnp.bfloat16)


def project(place, attn, weights, stream, down_weight):
    rows, width = stream.shape
    return pl.pallas_call(
        project_kernel,
        out_shape=(
            jax.ShapeDtypeStruct((ROWS, width), jnp.bfloat16),
            jax.ShapeDtypeStruct((2, rows, 320), jnp.float32),
            jax.ShapeDtypeStruct((2, rows, 320), jnp.bfloat16),
        ),
        in_specs=[SM] + [VM] * 8,
        out_specs=(VM, VM, VM),
        scratch_shapes=[pltpu.VMEM((rows, width), jnp.bfloat16)],
        cost_estimate=pl.CostEstimate(flops=4_000_000_000, bytes_accessed=7_000_000, transcendentals=0),
    )(place, attn, *weights, stream, down_weight)


def owner_kernel(place_ref, keep_ref, arrived_ref, here_ref, there_ref):
    first = keep_ref[0] + arrived_ref[0].astype(jnp.float32)
    second = keep_ref[1] + arrived_ref[1].astype(jnp.float32)
    near = place_ref[0] == 0
    here_ref[...] = jnp.where(near, first, second)
    there_ref[...] = jnp.where(near, second, first).astype(jnp.bfloat16)


def owner(place, keep, arrived):
    rows = keep.shape[1]
    return pl.pallas_call(
        owner_kernel,
        out_shape=(jax.ShapeDtypeStruct((rows, 320), jnp.float32), jax.ShapeDtypeStruct((rows, 320), jnp.bfloat16)),
        in_specs=[SM, VM, VM],
        out_specs=(VM, VM),
        cost_estimate=pl.CostEstimate(flops=1_000_000, bytes_accessed=900_000, transcendentals=0),
    )(place, keep, arrived)


def turned(value, axis, by):
    return lax.ppermute(value, axis, [(i, (i + by) % 4) for i in range(4)])


def line_halves(block):
    held = block
    for bit in (4, 2, 1):
        other = lax.ppermute(held, "z", [(i, i ^ bit) for i in range(8)])
        if bit == 1:
            return held, other
        held = jnp.concatenate([held, other], axis=0)


def plane_gathered(blocks):
    own = jnp.stack([blocks] + [turned(blocks, "x", k) for k in (1, 2, 3)])
    less, more = turned(own, "y", 1), turned(own, "y", -1)
    return own, less, more, turned(less[:, :, :16], "y", 1), turned(more[:, :, 16:], "y", -1)


def across(value, axis):
    return lax.ppermute(value, axis, [(0, 1), (1, 0)])


def on_device(queries, keys, values, patch_stream, out_weight, down_weight, byte_states, patch_starts):
    y, z, x, h, c = (lax.axis_index(a) for a in (*SEQ, *TP))
    starts = patch_starts.reshape(-1)
    pairs = [(a * 4 + t, t * 4 + a) for a in range(4) for t in range(4)]
    block = lax.ppermute(out_weight.T, ("y", "h", "c"), pairs)
    blocks = jnp.concatenate(line_halves(block[None]), axis=0)
    weights = plane_gathered(blocks)
    kv, last = prepare(patch_starts, keys, values, queries, patch_stream)
    earlier = lax.ppermute(last, SEQ, [(i, i + 1) for i in range(127)])
    near, far = line_halves(kv)
    q = jnp.concatenate([queries, earlier[:, :512], jnp.zeros((PAD - ROWS - 1, 512), jnp.bfloat16)], axis=0)
    stream = jnp.concatenate([patch_stream, earlier[:, 512:], jnp.zeros((PAD - ROWS - 1, 1024), jnp.bfloat16)], axis=0)
    q = exchange(jnp.broadcast_to(q[None], (16, *q.shape)), PLANE)

    place = jnp.stack([(y * 32 + x) * ROWS, z * 4]).astype(jnp.int32)
    slot = jnp.arange(8 * ROWS, dtype=jnp.int32)
    away = slot // ROWS
    away = (away & 1) * 4 + (away & 2) + (away >> 2)
    key_ids = ((away ^ z) * (4 * ROWS) + slot % ROWS)[None]
    parts = attend(place, key_ids, q, near, far)
    parts = exchange(parts, PLANE)
    attn = combine(parts)

    attn = lax.all_gather(attn, TP, axis=0)
    new_patches, keep, send = project(jnp.stack([y, x, c, z]), attn, weights, stream, down_weight)
    here, there = owner(h[None], keep, across(send, "c"))
    patch_down = (here + across(there, "h").astype(jnp.float32)).astype(jnp.bfloat16)

    position = jnp.arange(B_DEV, dtype=jnp.int32)[:, None]
    begins = jnp.concatenate([starts, jnp.zeros((1,), jnp.int32), jnp.full((PAD - ROWS - 1,), B_DEV, jnp.int32)])
    ends = jnp.concatenate([starts[1:], jnp.full((1,), B_DEV, jnp.int32), starts[:1], jnp.full((PAD - ROWS - 1,), B_DEV, jnp.int32)])
    member = ((begins[None, :] <= position) & (position < ends[None, :])).astype(jnp.bfloat16)
    added = jnp.dot(member, patch_down, preferred_element_type=jnp.float32)
    new_bytes = (byte_states.astype(jnp.float32) + added).astype(jnp.bfloat16)
    return (new_patches, new_bytes)


def solution(mesh):
    split = Mesh(mesh.devices.reshape(4, 8, 4, 2, 2), ("y", "z", "x", "h", "c"))
    return jax.shard_map(
        on_device,
        mesh=split,
        in_specs=(
            P(SEQ, TP),
            P(SEQ, TP),
            P(SEQ, TP),
            P(SEQ, TP),
            P(TP, SEQ),
            P(TP, None),
            P(SEQ, TP),
            P(SEQ, None),
        ),
        out_specs=(P(SEQ, TP), P(SEQ, TP)),
        check_vma=False,
    )
```

```python
import jax
import jax.numpy as jnp
from jax import lax
from jax.experimental import pallas as pl
from jax.experimental.pallas import tpu as pltpu
from jax.sharding import Mesh
from jax.sharding import PartitionSpec as P


DH = 128
B_DEV = 192
SEQ = ("y", "z", "x")
TP = ("h", "c")
PLANE = ("y", "x")
ROWS = 48
PAD = 56
NEG = -1e30
FLOOR = -1e29
MARK = 64.0
LIMIT = 4096.0
FAR = 1 << 30


def prepare_kernel(starts_ref, keys_ref, values_ref, queries_ref, stream_ref, kv_ref, last_ref):
    rows = keys_ref.shape[0]
    valid = (starts_ref[...] < B_DEV).astype(jnp.float32)
    count = jnp.sum(valid, axis=1, keepdims=True)
    row = lax.broadcasted_iota(jnp.int32, (rows, rows), 0)
    lane = lax.broadcasted_iota(jnp.int32, (rows, rows), 1)
    held = jnp.sum(jnp.where(row == lane, valid, 0.0), axis=1, keepdims=True)
    width = keys_ref.shape[1]
    kv_ref[0, :, :width] = jnp.where(held > 0, keys_ref[...], jnp.full_like(keys_ref, MARK))
    kv_ref[0, :, width:] = values_ref[...]
    lane = lax.broadcasted_iota(jnp.int32, (1, rows), 1).astype(jnp.float32)
    pick = (lane == count - 1).astype(jnp.bfloat16)
    last_ref[:, :width] = jnp.dot(pick, queries_ref[...], preferred_element_type=jnp.float32).astype(jnp.bfloat16)
    last_ref[:, width:] = jnp.dot(pick, stream_ref[...], preferred_element_type=jnp.float32).astype(jnp.bfloat16)


def attend_kernel(place_ref, key_ids_ref, q_ref, near_ref, far_ref, out_ref):
    blocks, rows, width = q_ref.shape
    heads = width // DH
    kv = jnp.concatenate([near_ref[...].reshape(-1, 2 * width), far_ref[...].reshape(-1, 2 * width)], axis=0)
    ones = jnp.ones((8, DH), jnp.bfloat16)
    nt = (((1,), (1,)), ((), ()))
    marks = lax.dot_general(ones, kv[:, :DH], nt, preferred_element_type=jnp.float32)[:1]
    key_ids = jnp.where(marks > LIMIT, FAR, key_ids_ref[...] + place_ref[0])
    group = 4
    row = lax.rem(lax.broadcasted_iota(jnp.int32, (group * rows, 1), 0), rows)
    step = lax.div(lax.broadcasted_iota(jnp.int32, (group * rows, 1), 0), rows)
    row = jnp.where(row < ROWS, row, -1) + step * ROWS
    lane = lax.broadcasted_iota(jnp.int32, (group * rows, DH), 1)

    def one_group(index, _):
        device = index * 32 + place_ref[1]
        allowed = key_ids <= row + device * ROWS
        stats = jnp.zeros((group * rows, DH), jnp.float32)
        at_blocks = pl.ds(index * group, group)
        for h in range(heads):
            q = q_ref[at_blocks, :, h * DH : (h + 1) * DH].reshape(group * rows, DH)
            k = kv[:, h * DH : (h + 1) * DH]
            v = kv[:, width + h * DH : width + (h + 1) * DH]
            s = lax.dot_general(q, k, nt, preferred_element_type=jnp.float32) * (DH**-0.5)
            s = jnp.where(allowed, s, NEG)
            peak = jnp.maximum(jnp.max(s, axis=1, keepdims=True), FLOOR).astype(jnp.bfloat16).astype(jnp.float32)
            e = jnp.exp(s - peak)
            total = jnp.sum(e, axis=1, keepdims=True)
            o = jnp.dot(e.astype(jnp.bfloat16), v, preferred_element_type=jnp.float32)
            out_ref[at_blocks, :, h * DH : (h + 1) * DH] = o.astype(jnp.bfloat16).reshape(group, rows, DH)
            coarse = total.astype(jnp.bfloat16).astype(jnp.float32)
            for at, part in enumerate((peak, coarse, total - coarse)):
                stats = jnp.where(lane == h * 3 + at, part, stats)
        out_ref[at_blocks, :, width:] = stats.astype(jnp.bfloat16).reshape(group, rows, DH)
        return 0

    lax.fori_loop(0, blocks // group, one_group, 0)


def combine_kernel(in_ref, out_ref):
    blocks, rows, width = in_ref.shape
    heads = (width - DH) // DH
    stats = [in_ref[b, :, heads * DH :].astype(jnp.float32) for b in range(blocks)]
    top = stats[0]
    for b in range(1, blocks):
        top = jnp.maximum(top, stats[b])
    shares = [jnp.exp(jnp.minimum(stat - top, 0.0)) for stat in stats]
    total = jnp.zeros_like(top)
    for share, stat in zip(shares, stats):
        total = total + share * (pltpu.roll(stat, DH - 1, 1) + pltpu.roll(stat, DH - 2, 1))
    scale = 1.0 / jnp.where(total > 0, total, 1.0)
    for h in range(heads):
        at = slice(h * DH, (h + 1) * DH)
        summed = jnp.zeros((rows, DH), jnp.float32)
        for b in range(blocks):
            summed = summed + shares[b][:, h * 3 : h * 3 + 1] * in_ref[b, :, at].astype(jnp.float32)
        out_ref[:, at] = (summed * scale[:, h * 3 : h * 3 + 1]).astype(jnp.bfloat16)


VM = pl.BlockSpec(memory_space=pltpu.VMEM)
SM = pl.BlockSpec(memory_space=pltpu.SMEM)


def prepare(starts, keys, values, queries, stream):
    rows, width = keys.shape
    return pl.pallas_call(
        prepare_kernel,
        out_shape=(
            jax.ShapeDtypeStruct((1, rows, 2 * width), jnp.bfloat16),
            jax.ShapeDtypeStruct((1, width + stream.shape[1]), jnp.bfloat16),
        ),
        in_specs=[VM] * 5,
        out_specs=(VM, VM),
        cost_estimate=pl.CostEstimate(flops=1_000_000, bytes_accessed=400_000, transcendentals=0),
    )(starts, keys, values, queries, stream)


def attend(place, key_ids, q, near, far):
    blocks, rows, width = q.shape
    return pl.pallas_call(
        attend_kernel,
        out_shape=jax.ShapeDtypeStruct((blocks, rows, width + DH), jnp.bfloat16),
        in_specs=[SM, VM, VM, VM, VM],
        out_specs=VM,
        cost_estimate=pl.CostEstimate(flops=4_000_000_000, bytes_accessed=3_000_000, transcendentals=1_400_000),
    )(place, key_ids, q, near, far)


def combine(parts):
    _, rows, width = parts.shape
    return pl.pallas_call(
        combine_kernel,
        out_shape=jax.ShapeDtypeStruct((rows, width - DH), jnp.bfloat16),
        in_specs=[VM],
        out_specs=VM,
        cost_estimate=pl.CostEstimate(flops=2_000_000_000, bytes_accessed=1_200_000, transcendentals=4_000),
    )(parts)


def exchange(value, axes):
    return lax.all_to_all(value, axes, split_axis=0, concat_axis=0, tiled=True)


def held_at(distance):
    return (distance & 1) * 4 + (distance & 2) + lax.div(distance, 4)


def project_kernel(place_ref, attn_ref, u0_ref, l0_ref, u1_ref, l1_ref, u2_ref, l2_ref, u3_ref, l3_ref, stream_ref, down_ref, out_ref, keep_ref, send_ref, new_ref):
    y, x, c, z = place_ref[0], place_ref[1], place_ref[2], place_ref[3]
    nt = (((1,), (1,)), ((), ()))
    span = 256
    heads = [attn_ref[lax.rem(y + step, 4)] for step in range(4)]
    turns = [lax.rem(x + 4 - source, 4) for source in range(4)]
    for at in range(stream_ref.shape[1] // span):
        total = stream_ref[:, at * span : (at + 1) * span].astype(jnp.float32)
        spots = [(turn, held_at((at * 2 + i) ^ z)) for i in range(2) for turn in turns]
        mixed = jnp.zeros_like(total)
        for attn, refs in zip(heads, ((u0_ref, l0_ref), (u1_ref, l1_ref), (u2_ref, l2_ref), (u3_ref, l3_ref))):
            weight = jnp.concatenate([ref[turn, spot] for turn, spot in spots for ref in refs], axis=0)
            mixed = mixed + lax.dot_general(attn, weight, nt, preferred_element_type=jnp.float32)
        new_ref[:, at * span : (at + 1) * span] = (total + mixed).astype(jnp.bfloat16)
    out_ref[...] = new_ref[:ROWS]
    down = jnp.dot(new_ref[...], down_ref[...], preferred_element_type=jnp.float32)
    for half in range(2):
        at = half * 640
        first, second = down[:, at : at + 320], down[:, at + 320 : at + 640]
        keep_ref[half] = jnp.where(c == 0, first, second)
        send_ref[half] = jnp.where(c == 0, second, first).astype(jnp.bfloat16)


def project(place, attn, weights, stream, down_weight):
    rows, width = stream.shape
    return pl.pallas_call(
        project_kernel,
        out_shape=(
            jax.ShapeDtypeStruct((ROWS, width), jnp.bfloat16),
            jax.ShapeDtypeStruct((2, rows, 320), jnp.float32),
            jax.ShapeDtypeStruct((2, rows, 320), jnp.bfloat16),
        ),
        in_specs=[SM] + [VM] * 11,
        out_specs=(VM, VM, VM),
        scratch_shapes=[pltpu.VMEM((rows, width), jnp.bfloat16)],
        cost_estimate=pl.CostEstimate(flops=4_000_000_000, bytes_accessed=7_000_000, transcendentals=0),
    )(place, attn, *weights, stream, down_weight)


def owner_kernel(place_ref, keep_ref, arrived_ref, here_ref, there_ref):
    first = keep_ref[0] + arrived_ref[0].astype(jnp.float32)
    second = keep_ref[1] + arrived_ref[1].astype(jnp.float32)
    near = place_ref[0] == 0
    here_ref[...] = jnp.where(near, first, second)
    there_ref[...] = jnp.where(near, second, first).astype(jnp.bfloat16)


def owner(place, keep, arrived):
    rows = keep.shape[1]
    return pl.pallas_call(
        owner_kernel,
        out_shape=(jax.ShapeDtypeStruct((rows, 320), jnp.float32), jax.ShapeDtypeStruct((rows, 320), jnp.bfloat16)),
        in_specs=[SM, VM, VM],
        out_specs=(VM, VM),
        cost_estimate=pl.CostEstimate(flops=1_000_000, bytes_accessed=900_000, transcendentals=0),
    )(place, keep, arrived)


def turned(value, axis, by):
    return lax.ppermute(value, axis, [(i, (i + by) % 4) for i in range(4)])


def line_halves(block):
    held = block
    for bit in (4, 2, 1):
        other = lax.ppermute(held, "z", [(i, i ^ bit) for i in range(8)])
        if bit == 1:
            return held, other
        held = jnp.concatenate([held, other], axis=0)


def plane_gathered(blocks):
    held = [blocks] + [turned(blocks, "x", k) for k in (1, 2, 3)]
    upper = jnp.stack([block[:, :16] for block in held])
    lower = jnp.stack([block[:, 16:] for block in held])
    less_upper, more_lower = turned(upper, "y", 1), turned(lower, "y", -1)
    less_lower, more_upper = turned(lower, "y", 1), turned(upper, "y", -1)
    far_upper, far_lower = turned(less_upper, "y", 1), turned(more_lower, "y", -1)
    return upper, lower, more_upper, more_lower, far_upper, far_lower, less_upper, less_lower


def across(value, axis):
    return lax.ppermute(value, axis, [(0, 1), (1, 0)])


def on_device(queries, keys, values, patch_stream, out_weight, down_weight, byte_states, patch_starts):
    y, z, x, h, c = (lax.axis_index(a) for a in (*SEQ, *TP))
    starts = patch_starts.reshape(-1)
    pairs = [(a * 4 + t, t * 4 + a) for a in range(4) for t in range(4)]
    block = lax.ppermute(out_weight.T, ("y", "h", "c"), pairs)
    blocks = jnp.concatenate(line_halves(block[None]), axis=0)
    weights = plane_gathered(blocks)
    kv, last = prepare(patch_starts, keys, values, queries, patch_stream)
    earlier = lax.ppermute(last, SEQ, [(i, i + 1) for i in range(127)])
    near, far = line_halves(kv)
    q = jnp.concatenate([queries, earlier[:, :512], jnp.zeros((PAD - ROWS - 1, 512), jnp.bfloat16)], axis=0)
    stream = jnp.concatenate([patch_stream, earlier[:, 512:], jnp.zeros((PAD - ROWS - 1, 1024), jnp.bfloat16)], axis=0)
    q = exchange(jnp.broadcast_to(q[None], (16, *q.shape)), PLANE)

    place = jnp.stack([(y * 32 + x) * ROWS, z * 4]).astype(jnp.int32)
    slot = jnp.arange(8 * ROWS, dtype=jnp.int32)
    away = slot // ROWS
    away = (away & 1) * 4 + (away & 2) + (away >> 2)
    key_ids = ((away ^ z) * (4 * ROWS) + slot % ROWS)[None]
    parts = attend(place, key_ids, q, near, far)
    parts = exchange(parts, PLANE)
    attn = combine(parts)

    attn = lax.all_gather(attn, TP, axis=0)
    new_patches, keep, send = project(jnp.stack([y, x, c, z]), attn, weights, stream, down_weight)
    here, there = owner(h[None], keep, across(send, "c"))
    patch_down = (here + across(there, "h").astype(jnp.float32)).astype(jnp.bfloat16)

    position = jnp.arange(B_DEV, dtype=jnp.int32)[:, None]
    begins = jnp.concatenate([starts, jnp.zeros((1,), jnp.int32), jnp.full((PAD - ROWS - 1,), B_DEV, jnp.int32)])
    ends = jnp.concatenate([starts[1:], jnp.full((1,), B_DEV, jnp.int32), starts[:1], jnp.full((PAD - ROWS - 1,), B_DEV, jnp.int32)])
    member = ((begins[None, :] <= position) & (position < ends[None, :])).astype(jnp.bfloat16)
    added = jnp.dot(member, patch_down, preferred_element_type=jnp.float32)
    new_bytes = (byte_states.astype(jnp.float32) + added).astype(jnp.bfloat16)
    return (new_patches, new_bytes)


def solution(mesh):
    split = Mesh(mesh.devices.reshape(4, 8, 4, 2, 2), ("y", "z", "x", "h", "c"))
    return jax.shard_map(
        on_device,
        mesh=split,
        in_specs=(
            P(SEQ, TP),
            P(SEQ, TP),
            P(SEQ, TP),
            P(SEQ, TP),
            P(TP, SEQ),
            P(TP, None),
            P(SEQ, TP),
            P(SEQ, None),
        ),
        out_specs=(P(SEQ, TP), P(SEQ, TP)),
        check_vma=False,
    )
```

```python
import jax
import jax.numpy as jnp
from jax import lax
from jax.experimental import pallas as pl
from jax.experimental.pallas import tpu as pltpu
from jax.sharding import Mesh
from jax.sharding import PartitionSpec as P


DH = 128
B_DEV = 192
SEQ = ("y", "z", "x")
TP = ("h", "c")
PLANE = ("y", "x")
ROWS = 48
PAD = 56
NEG = -1e30
LOG2E = 1.4426950408889634
FLOOR = -1e29
MARK = 64.0
LIMIT = 4096.0
FAR = 1 << 30


def prepare_kernel(starts_ref, keys_ref, values_ref, queries_ref, stream_ref, kv_ref, last_ref):
    rows = keys_ref.shape[0]
    valid = (starts_ref[...] < B_DEV).astype(jnp.float32)
    count = jnp.sum(valid, axis=1, keepdims=True)
    row = lax.broadcasted_iota(jnp.int32, (rows, rows), 0)
    lane = lax.broadcasted_iota(jnp.int32, (rows, rows), 1)
    held = jnp.sum(jnp.where(row == lane, valid, 0.0), axis=1, keepdims=True)
    width = keys_ref.shape[1]
    kv_ref[0, :, :width] = jnp.where(held > 0, keys_ref[...], jnp.full_like(keys_ref, MARK))
    kv_ref[0, :, width:] = values_ref[...]
    lane = lax.broadcasted_iota(jnp.int32, (1, rows), 1).astype(jnp.float32)
    pick = (lane == count - 1).astype(jnp.bfloat16)
    last_ref[:, :width] = jnp.dot(pick, queries_ref[...], preferred_element_type=jnp.float32).astype(jnp.bfloat16)
    last_ref[:, width:] = jnp.dot(pick, stream_ref[...], preferred_element_type=jnp.float32).astype(jnp.bfloat16)


def attend_kernel(place_ref, key_ids_ref, q_ref, near_ref, far_ref, out_ref):
    blocks, rows, width = q_ref.shape
    heads = width // DH
    kv = jnp.concatenate([near_ref[...].reshape(-1, 2 * width), far_ref[...].reshape(-1, 2 * width)], axis=0)
    ones = jnp.ones((8, DH), jnp.bfloat16)
    nt = (((1,), (1,)), ((), ()))
    marks = lax.dot_general(ones, kv[:, :DH], nt, preferred_element_type=jnp.float32)[:1]
    key_ids = jnp.where(marks > LIMIT, FAR, key_ids_ref[...] + place_ref[0])
    group = 4
    row = lax.rem(lax.broadcasted_iota(jnp.int32, (group * rows, 1), 0), rows)
    step = lax.div(lax.broadcasted_iota(jnp.int32, (group * rows, 1), 0), rows)
    row = jnp.where(row < ROWS, row, -1) + step * ROWS
    lane = lax.broadcasted_iota(jnp.int32, (group * rows, DH), 1)

    def one_group(index, _):
        device = index * 32 + place_ref[1]
        allowed = key_ids <= row + device * ROWS
        stats = jnp.zeros((group * rows, DH), jnp.float32)
        at_blocks = pl.ds(index * group, group)
        for h in range(heads):
            q = q_ref[at_blocks, :, h * DH : (h + 1) * DH].reshape(group * rows, DH)
            k = kv[:, h * DH : (h + 1) * DH]
            v = kv[:, width + h * DH : width + (h + 1) * DH]
            s = lax.dot_general(q, k, nt, preferred_element_type=jnp.float32) * (DH**-0.5 * LOG2E)
            s = jnp.where(allowed, s, NEG)
            peak = jnp.maximum(jnp.max(s, axis=1, keepdims=True), FLOOR).astype(jnp.bfloat16).astype(jnp.float32)
            e = jnp.exp2(s - peak)
            total = jnp.sum(e, axis=1, keepdims=True)
            o = jnp.dot(e.astype(jnp.bfloat16), v, preferred_element_type=jnp.float32)
            out_ref[at_blocks, :, h * DH : (h + 1) * DH] = o.astype(jnp.bfloat16).reshape(group, rows, DH)
            coarse = total.astype(jnp.bfloat16).astype(jnp.float32)
            for at, part in enumerate((peak, coarse, total - coarse)):
                stats = jnp.where(lane == h * 3 + at, part, stats)
        out_ref[at_blocks, :, width:] = stats.astype(jnp.bfloat16).reshape(group, rows, DH)
        return 0

    lax.fori_loop(0, blocks // group, one_group, 0)


def combine_kernel(in_ref, out_ref):
    blocks, rows, width = in_ref.shape
    heads = (width - DH) // DH
    stats = [in_ref[b, :, heads * DH :].astype(jnp.float32) for b in range(blocks)]
    top = stats[0]
    for b in range(1, blocks):
        top = jnp.maximum(top, stats[b])
    shares = [jnp.exp2(jnp.minimum(stat - top, 0.0)) for stat in stats]
    total = jnp.zeros_like(top)
    for share, stat in zip(shares, stats):
        total = total + share * (pltpu.roll(stat, DH - 1, 1) + pltpu.roll(stat, DH - 2, 1))
    scale = 1.0 / jnp.where(total > 0, total, 1.0)
    for h in range(heads):
        at = slice(h * DH, (h + 1) * DH)
        summed = jnp.zeros((rows, DH), jnp.float32)
        for b in range(blocks):
            summed = summed + shares[b][:, h * 3 : h * 3 + 1] * in_ref[b, :, at].astype(jnp.float32)
        out_ref[:, at] = (summed * scale[:, h * 3 : h * 3 + 1]).astype(jnp.bfloat16)


VM = pl.BlockSpec(memory_space=pltpu.VMEM)
SM = pl.BlockSpec(memory_space=pltpu.SMEM)


def prepare(starts, keys, values, queries, stream):
    rows, width = keys.shape
    return pl.pallas_call(
        prepare_kernel,
        out_shape=(
            jax.ShapeDtypeStruct((1, rows, 2 * width), jnp.bfloat16),
            jax.ShapeDtypeStruct((1, width + stream.shape[1]), jnp.bfloat16),
        ),
        in_specs=[VM] * 5,
        out_specs=(VM, VM),
        cost_estimate=pl.CostEstimate(flops=1_000_000, bytes_accessed=400_000, transcendentals=0),
    )(starts, keys, values, queries, stream)


def attend(place, key_ids, q, near, far):
    blocks, rows, width = q.shape
    return pl.pallas_call(
        attend_kernel,
        out_shape=jax.ShapeDtypeStruct((blocks, rows, width + DH), jnp.bfloat16),
        in_specs=[SM, VM, VM, VM, VM],
        out_specs=VM,
        cost_estimate=pl.CostEstimate(flops=4_000_000_000, bytes_accessed=3_000_000, transcendentals=1_400_000),
    )(place, key_ids, q, near, far)


def combine(parts):
    _, rows, width = parts.shape
    return pl.pallas_call(
        combine_kernel,
        out_shape=jax.ShapeDtypeStruct((rows, width - DH), jnp.bfloat16),
        in_specs=[VM],
        out_specs=VM,
        cost_estimate=pl.CostEstimate(flops=2_000_000_000, bytes_accessed=1_200_000, transcendentals=4_000),
    )(parts)


def exchange(value, axes):
    return lax.all_to_all(value, axes, split_axis=0, concat_axis=0, tiled=True)


def held_at(distance):
    return (distance & 1) * 4 + (distance & 2) + lax.div(distance, 4)


def project_kernel(place_ref, attn_ref, u0_ref, l0_ref, u1_ref, l1_ref, u2_ref, l2_ref, u3_ref, l3_ref, stream_ref, down_ref, out_ref, keep_ref, send_ref, new_ref):
    y, x, c, z = place_ref[0], place_ref[1], place_ref[2], place_ref[3]
    nt = (((1,), (1,)), ((), ()))
    span = 256
    heads = [attn_ref[lax.rem(y + step, 4)] for step in range(4)]
    turns = [lax.rem(x + 4 - source, 4) for source in range(4)]
    for at in range(stream_ref.shape[1] // span):
        total = stream_ref[:, at * span : (at + 1) * span].astype(jnp.float32)
        spots = [(turn, held_at((at * 2 + i) ^ z)) for i in range(2) for turn in turns]
        mixed = jnp.zeros_like(total)
        for attn, refs in zip(heads, ((u0_ref, l0_ref), (u1_ref, l1_ref), (u2_ref, l2_ref), (u3_ref, l3_ref))):
            weight = jnp.concatenate([ref[turn, spot] for turn, spot in spots for ref in refs], axis=0)
            mixed = mixed + lax.dot_general(attn, weight, nt, preferred_element_type=jnp.float32)
        new_ref[:, at * span : (at + 1) * span] = (total + mixed).astype(jnp.bfloat16)
    out_ref[...] = new_ref[:ROWS]
    down = jnp.dot(new_ref[...], down_ref[...], preferred_element_type=jnp.float32)
    for half in range(2):
        at = half * 640
        first, second = down[:, at : at + 320], down[:, at + 320 : at + 640]
        keep_ref[half] = jnp.where(c == 0, first, second)
        send_ref[half] = jnp.where(c == 0, second, first).astype(jnp.bfloat16)


def project(place, attn, weights, stream, down_weight):
    rows, width = stream.shape
    return pl.pallas_call(
        project_kernel,
        out_shape=(
            jax.ShapeDtypeStruct((ROWS, width), jnp.bfloat16),
            jax.ShapeDtypeStruct((2, rows, 320), jnp.float32),
            jax.ShapeDtypeStruct((2, rows, 320), jnp.bfloat16),
        ),
        in_specs=[SM] + [VM] * 11,
        out_specs=(VM, VM, VM),
        scratch_shapes=[pltpu.VMEM((rows, width), jnp.bfloat16)],
        cost_estimate=pl.CostEstimate(flops=4_000_000_000, bytes_accessed=7_000_000, transcendentals=0),
    )(place, attn, *weights, stream, down_weight)


def owner_kernel(place_ref, keep_ref, arrived_ref, here_ref, there_ref):
    first = keep_ref[0] + arrived_ref[0].astype(jnp.float32)
    second = keep_ref[1] + arrived_ref[1].astype(jnp.float32)
    near = place_ref[0] == 0
    here_ref[...] = jnp.where(near, first, second)
    there_ref[...] = jnp.where(near, second, first).astype(jnp.bfloat16)


def owner(place, keep, arrived):
    rows = keep.shape[1]
    return pl.pallas_call(
        owner_kernel,
        out_shape=(jax.ShapeDtypeStruct((rows, 320), jnp.float32), jax.ShapeDtypeStruct((rows, 320), jnp.bfloat16)),
        in_specs=[SM, VM, VM],
        out_specs=(VM, VM),
        cost_estimate=pl.CostEstimate(flops=1_000_000, bytes_accessed=900_000, transcendentals=0),
    )(place, keep, arrived)


def turned(value, axis, by):
    return lax.ppermute(value, axis, [(i, (i + by) % 4) for i in range(4)])


def line_halves(block):
    held = block
    for bit in (4, 2, 1):
        other = lax.ppermute(held, "z", [(i, i ^ bit) for i in range(8)])
        if bit == 1:
            return held, other
        held = jnp.concatenate([held, other], axis=0)


def plane_gathered(blocks):
    held = [blocks] + [turned(blocks, "x", k) for k in (1, 2, 3)]
    upper = jnp.stack([block[:, :16] for block in held])
    lower = jnp.stack([block[:, 16:] for block in held])
    less_upper, more_lower = turned(upper, "y", 1), turned(lower, "y", -1)
    less_lower, more_upper = turned(lower, "y", 1), turned(upper, "y", -1)
    far_upper, far_lower = turned(less_upper, "y", 1), turned(more_lower, "y", -1)
    return upper, lower, more_upper, more_lower, far_upper, far_lower, less_upper, less_lower


def across(value, axis):
    return lax.ppermute(value, axis, [(0, 1), (1, 0)])


def on_device(queries, keys, values, patch_stream, out_weight, down_weight, byte_states, patch_starts):
    y, z, x, h, c = (lax.axis_index(a) for a in (*SEQ, *TP))
    starts = patch_starts.reshape(-1)
    pairs = [(a * 4 + t, t * 4 + a) for a in range(4) for t in range(4)]
    block = lax.ppermute(out_weight.T, ("y", "h", "c"), pairs)
    blocks = jnp.concatenate(line_halves(block[None]), axis=0)
    weights = plane_gathered(blocks)
    kv, last = prepare(patch_starts, keys, values, queries, patch_stream)
    earlier = lax.ppermute(last, SEQ, [(i, i + 1) for i in range(127)])
    near, far = line_halves(kv)
    q = jnp.concatenate([queries, earlier[:, :512], jnp.zeros((PAD - ROWS - 1, 512), jnp.bfloat16)], axis=0)
    stream = jnp.concatenate([patch_stream, earlier[:, 512:], jnp.zeros((PAD - ROWS - 1, 1024), jnp.bfloat16)], axis=0)
    q = exchange(jnp.broadcast_to(q[None], (16, *q.shape)), PLANE)

    place = jnp.stack([(y * 32 + x) * ROWS, z * 4]).astype(jnp.int32)
    slot = jnp.arange(8 * ROWS, dtype=jnp.int32)
    away = slot // ROWS
    away = (away & 1) * 4 + (away & 2) + (away >> 2)
    key_ids = ((away ^ z) * (4 * ROWS) + slot % ROWS)[None]
    parts = attend(place, key_ids, q, near, far)
    parts = exchange(parts, PLANE)
    attn = combine(parts)

    attn = lax.all_gather(attn, TP, axis=0)
    new_patches, keep, send = project(jnp.stack([y, x, c, z]), attn, weights, stream, down_weight)
    here, there = owner(h[None], keep, across(send, "c"))
    patch_down = (here + across(there, "h").astype(jnp.float32)).astype(jnp.bfloat16)

    position = jnp.arange(B_DEV, dtype=jnp.int32)[:, None]
    begins = jnp.concatenate([starts, jnp.zeros((1,), jnp.int32), jnp.full((PAD - ROWS - 1,), B_DEV, jnp.int32)])
    ends = jnp.concatenate([starts[1:], jnp.full((1,), B_DEV, jnp.int32), starts[:1], jnp.full((PAD - ROWS - 1,), B_DEV, jnp.int32)])
    member = ((begins[None, :] <= position) & (position < ends[None, :])).astype(jnp.bfloat16)
    added = jnp.dot(member, patch_down, preferred_element_type=jnp.float32)
    new_bytes = (byte_states.astype(jnp.float32) + added).astype(jnp.bfloat16)
    return (new_patches, new_bytes)


def solution(mesh):
    split = Mesh(mesh.devices.reshape(4, 8, 4, 2, 2), ("y", "z", "x", "h", "c"))
    return jax.shard_map(
        on_device,
        mesh=split,
        in_specs=(
            P(SEQ, TP),
            P(SEQ, TP),
            P(SEQ, TP),
            P(SEQ, TP),
            P(TP, SEQ),
            P(TP, None),
            P(SEQ, TP),
            P(SEQ, None),
        ),
        out_specs=(P(SEQ, TP), P(SEQ, TP)),
        check_vma=False,
    )
```
